32 devices in a mesh: src: 4 (over z), rcv: 8 (over y, x, core).
Axes of the slice: x: 2, y: 2, z: 4, core: 2. Of those that a mesh axis runs over, the one named last changes fastest.
Arguments:
- traces: bfloat16 [512, 2048, 512], P('src', 'rcv'), may hold values from -6 to 6
- virtual_source_index: int32 [256], replicated, may hold values from 0 to 2047
Outputs:
- correlations: float32 [256, 2048, 512], P('rcv', 'src')
The draws below stay inside these ranges and needn't reach their ends.
Inputs may be any that keep to these rules, and one draw needn't show every extreme that they name: `virtual_source_index`: receiver numbers; a receiver may be listed more than once.
All inputs are finite; a program needn't handle non-finite values.
Results may differ from the reference program's by a relative error of at most 0.0064.
Values may be sent and summed in bfloat16 or wider, within the bound.
No kernel may reach another device: no remote copies, remote signals or barrier semaphores. Data moves between devices by JAX's collectives and lax.ppermute only.
A program may use at most 192 MiB of HBM per device.

```python
import math
import jax
import jax.numpy as jnp
from jax import lax

NT = 512
NF = 128
RCV = 2048
VS = 256
SHOTS = 512


def place_ends(array, stream_key, smallest, top_value):
    dims = array.shape
    place = [jax.random.randint(jax.random.fold_in(stream_key, axis), (), 0, dims[axis]) for axis in range(len(dims))]
    array = array.at[tuple(place)].set(smallest)
    longest = dims.index(max(dims))
    place[longest] = (place[longest] + 1) % dims[longest]
    return array.at[tuple(place)].set(top_value)


def shard_levels(key, dims, pieces, least, high):
    loudness = 1.0
    for position, shards_of in pieces:
        steps = jax.random.uniform(jax.random.fold_in(jax.random.fold_in(key, 6), position), (shards_of,), jnp.float32, least / len(pieces), high / len(pieces))
        loudness = loudness * jnp.repeat(jnp.exp(steps), dims[position] // shards_of).reshape((-1,) + (1,) * (len(dims) - 1 - position))
    return loudness


def noise(own_key, shape, width, most, split=(), kind=jnp.bfloat16):
    entries = jax.random.normal(own_key, shape, jnp.float32) * width
    if len(split) > 0:
        entries = shard_levels(own_key, shape, split, -0.22, 0.18) * entries
    return jnp.clip(entries, min=-most, max=most).astype(kind)


def setup_inputs(seed: int = 0) -> dict:
    streams_of = jax.random.split(jax.random.key(seed), 3)
    return {
        "traces": noise(streams_of[0], (SHOTS, RCV, NT), 1.0, 6.0, ((0, 4), (1, 8))),
        "virtual_source_index": place_ends(jax.random.randint(streams_of[1], (VS,), 0, RCV), jax.random.fold_in(streams_of[1], 1), 0, RCV - 1).astype(jnp.int32),
    }


def make_tables():
    freqs = jnp.arange(NF, dtype=jnp.int32)
    times = jnp.arange(NT, dtype=jnp.int32)
    phase = (freqs[:, None] * times[None, :] % NT).astype(jnp.float32) * (2.0 * math.pi / NT)
    basis = jnp.stack([jnp.cos(phase), -jnp.sin(phase)], axis=1)
    forward = (basis / jnp.sqrt(jnp.float32(NT))).astype(jnp.bfloat16)
    inverse = (basis / jnp.sqrt(jnp.float32(NF))).astype(jnp.bfloat16)
    return (forward, inverse)

def complex_gram(left_operand, right_operand):
    high_precision = lax.Precision.HIGHEST
    real_part = jnp.einsum('ekg,ekh->egh', left_operand[:, 0], right_operand[:, 0], precision=high_precision) + jnp.einsum('ekg,ekh->egh', left_operand[:, 1], right_operand[:, 1], precision=high_precision)
    imaginary_part = jnp.einsum('ekg,ekh->egh', left_operand[:, 0], right_operand[:, 1], precision=high_precision) - jnp.einsum('ekg,ekh->egh', left_operand[:, 1], right_operand[:, 0], precision=high_precision)
    return jnp.stack([real_part, imaginary_part], axis=1)

def reference(traces, virtual_source_index):
    forward, inverse = make_tables()
    frequency_block = 8
    flat = traces.reshape(SHOTS * RCV, NT)
    scale = 1.0 / jnp.sqrt(jnp.float32(SHOTS))

    def one_block(table):
        spec = jnp.dot(flat, table.reshape(frequency_block * 2, NT).T, preferred_element_type=jnp.float32)
        spec = spec.astype(jnp.bfloat16).reshape(SHOTS, RCV, frequency_block, 2).transpose(2, 3, 0, 1).astype(jnp.float32)
        rows = jnp.take(spec, virtual_source_index, axis=3)
        gram = complex_gram(rows, spec) * scale
        return gram.astype(jnp.bfloat16)
    scaled = lax.map(one_block, forward.reshape(NF // frequency_block, frequency_block, 2, NT))
    scaled = scaled.reshape(NF, 2, VS, RCV).transpose(2, 0, 1, 3)
    inverse_flattened = inverse.reshape(2 * NF, NT)

    def one_source(block):
        return jnp.dot(block.reshape(2 * NF, RCV).T, inverse_flattened, preferred_element_type=jnp.float32)
    return lax.map(one_source, scaled)
```

```python
import functools
import math

import jax
import jax.numpy as jnp
from jax import lax
from jax.experimental import pallas as pl
from jax.experimental.pallas import tpu as pltpu
from jax.sharding import PartitionSpec as P


NF = 128


def make_tables(times_count):
    freqs = jnp.arange(NF, dtype=jnp.int32)
    times = jnp.arange(times_count, dtype=jnp.int32)
    phase = (freqs[:, None] * times[None, :] % times_count).astype(jnp.float32) * (
        2.0 * math.pi / times_count
    )
    basis = jnp.stack([jnp.cos(phase), -jnp.sin(phase)], axis=1)
    forward = (basis / jnp.sqrt(jnp.float32(times_count))).astype(jnp.bfloat16)
    inverse = (basis / jnp.sqrt(jnp.float32(NF))).astype(jnp.bfloat16)
    return (forward, inverse)


def left_operands(rows):
    return jnp.concatenate(
        [
            jnp.concatenate([rows[0], rows[1]], axis=1),
            jnp.concatenate([-rows[1], rows[0]], axis=1),
        ],
        axis=0,
    )


def gram_body(scale, sources, *refs):
    rows, cols, out = refs[:sources], refs[sources : 2 * sources], refs[-1]
    left = [left_operands(r) for r in rows]
    per, _, shots, rcv = cols[0].shape
    owners, _, _, vs, _ = out.shape
    for h in range(per):
        total = None
        for a, c in zip(left, cols):
            part = jnp.dot(a, c[h].reshape(2 * shots, rcv), preferred_element_type=jnp.float32)
            total = part if total is None else total + part
        total = (total * scale).astype(out.dtype)
        for c in range(2):
            for o in range(owners):
                at = (c * owners + o) * vs
                out[o, 0, c, :, h * rcv : (h + 1) * rcv] = total[at : at + vs]


def gram(rows, cols, owners, scale):
    k, vs, shots = rows[0].shape
    per, _, _, rcv = cols[0].shape
    flops = len(rows) * 2 * (2 * vs) * shots * per * rcv * k
    moved = len(rows) * 2 * k * shots * (vs + per * rcv) + 2 * k * vs * per * rcv
    return pl.pallas_call(
        functools.partial(gram_body, scale, len(rows)),
        grid=(k // 2,),
        in_specs=[pl.BlockSpec((2, vs, shots), lambda f: (f, 0, 0))] * len(rows)
        + [pl.BlockSpec((per, 2, shots, rcv), lambda f: (0, f, 0, 0))] * len(rows),
        out_specs=pl.BlockSpec((owners, 1, 2, vs // owners, per * rcv), lambda f: (0, f, 0, 0, 0)),
        out_shape=jax.ShapeDtypeStruct((owners, k // 2, 2, vs // owners, per * rcv), jnp.bfloat16),
        cost_estimate=pl.CostEstimate(flops=flops, bytes_accessed=moved, transcendentals=0),
        name="gram",
    )(*rows, *cols)


def lags_body(pieces, *refs):
    table, out = refs[pieces], refs[-1]
    for v in range(out.shape[0]):
        spectra = jnp.concatenate([refs[p][v] for p in range(pieces)], axis=0)
        out[v] = lax.dot_general(
            spectra, table[...], (((0,), (0,)), ((), ())), preferred_element_type=jnp.float32
        )


def lags(pieces, table):
    vs, _, rcv = pieces[0].shape
    k, times = table.shape
    step = 2
    return pl.pallas_call(
        functools.partial(lags_body, len(pieces)),
        grid=(vs // step,),
        in_specs=[pl.BlockSpec((step,) + p.shape[1:], lambda v: (v, 0, 0)) for p in pieces]
        + [pl.BlockSpec((k, times), lambda v: (0, 0))],
        out_specs=pl.BlockSpec((step, rcv, times), lambda v: (v, 0, 0)),
        out_shape=jax.ShapeDtypeStruct((vs, rcv, times), jnp.float32),
        cost_estimate=pl.CostEstimate(
            flops=2 * vs * rcv * times * k,
            bytes_accessed=2 * vs * rcv * k + 4 * vs * rcv * times,
            transcendentals=0,
        ),
        name="lags",
    )(*pieces, table)


def signed_product(left, cols, h):
    _, _, shots, rcv = cols.shape
    return jnp.dot(left, cols[h].reshape(2 * shots, rcv), preferred_element_type=jnp.float32)


def cross_body(scale, sel, own_rows, end_rows, own_cols, end_cols, out):
    rcv = own_cols.shape[3]
    own, end = left_operands(own_rows), left_operands(end_rows)
    for h in range(own_cols.shape[0]):
        total = signed_product(own, own_cols, h) + signed_product(end, end_cols, h)
        out[0, 0, :, h * rcv : (h + 1) * rcv] = (total * scale).astype(out.dtype)


def cross(sel, own_rows, end_rows, own_cols, end_cols, per, scale):
    k, vs, shots = own_rows.shape
    rcv = own_cols.shape[3]
    rows = pl.BlockSpec((2, vs, shots), lambda f, m, sel: (f, 0, 0))
    return pl.pallas_call(
        functools.partial(cross_body, scale),
        grid_spec=pltpu.PrefetchScalarGridSpec(
            num_scalar_prefetch=1,
            grid=(k // 2, 2),
            in_specs=[
                rows,
                rows,
                pl.BlockSpec((per, 2, shots, rcv), lambda f, m, sel: (2 * sel[0] + m, f, 0, 0)),
                pl.BlockSpec((per, 2, shots, rcv), lambda f, m, sel: (sel[0] + m, f, 0, 0)),
            ],
            out_specs=pl.BlockSpec((1, 1, 2 * vs, per * rcv), lambda f, m, sel: (m, f, 0, 0)),
        ),
        out_shape=jax.ShapeDtypeStruct((2, k // 2, 2 * vs, per * rcv), jnp.bfloat16),
        cost_estimate=pl.CostEstimate(
            flops=16 * k * vs * shots * per * rcv,
            bytes_accessed=4 * k * (vs * shots + 2 * shots * per * rcv + vs * per * rcv),
            transcendentals=0,
        ),
        name="cross",
    )(sel, own_rows, end_rows, own_cols, end_cols)


def onward_body(scale, sel, own_rows, own_cols, far, out):
    rcv = own_cols.shape[3]
    own = left_operands(own_rows)
    for h in range(own_cols.shape[0]):
        at = slice(h * rcv, (h + 1) * rcv)
        total = signed_product(own, own_cols, h) * scale + far[0, 0, :, at].astype(jnp.float32)
        out[0, :, at] = total.astype(out.dtype)


def onward(sel, own_rows, own_cols, crossed, per, scale):
    k, vs, shots = own_rows.shape
    rcv = own_cols.shape[3]
    return pl.pallas_call(
        functools.partial(onward_body, scale),
        grid_spec=pltpu.PrefetchScalarGridSpec(
            num_scalar_prefetch=1,
            grid=(k // 2,),
            in_specs=[
                pl.BlockSpec((2, vs, shots), lambda f, sel: (f, 0, 0)),
                pl.BlockSpec((per, 2, shots, rcv), lambda f, sel: (3 - 3 * sel[0], f, 0, 0)),
                pl.BlockSpec((1, 1, 2 * vs, per * rcv), lambda f, sel: (1 - sel[0], f, 0, 0)),
            ],
            out_specs=pl.BlockSpec((1, 2 * vs, per * rcv), lambda f, sel: (f, 0, 0)),
        ),
        out_shape=jax.ShapeDtypeStruct((k // 2, 2 * vs, per * rcv), jnp.bfloat16),
        cost_estimate=pl.CostEstimate(
            flops=4 * k * vs * shots * per * rcv,
            bytes_accessed=2 * k * (vs * shots + shots * per * rcv + 2 * vs * per * rcv),
            transcendentals=0,
        ),
        name="onward",
    )(sel, own_rows, own_cols, crossed)


def finish_body(scale, sel, own_rows, end_rows, own_cols, end_cols, near, mine, arrived, out):
    owners, _, _, vs, _ = out.shape
    rcv = own_cols.shape[3]

    def put(h, total):
        total = total.astype(out.dtype)
        for c in range(2):
            for o in range(owners):
                at = (c * owners + o) * vs
                out[o, 0, c, :, h * rcv : (h + 1) * rcv] = total[at : at + vs]

    @pl.when(sel[2] == 1)
    def _():
        own, end = left_operands(own_rows), left_operands(end_rows)
        for h in range(own_cols.shape[0]):
            total = signed_product(own, own_cols, h) + signed_product(end, end_cols, h)
            at = slice(h * rcv, (h + 1) * rcv)
            put(h, total * scale + near[0, 0, :, at].astype(jnp.float32))

    @pl.when(sel[2] == 0)
    def _():
        for h in range(own_cols.shape[0]):
            at = slice(h * rcv, (h + 1) * rcv)
            put(h, mine[0, :, at].astype(jnp.float32) + arrived[0, :, at].astype(jnp.float32))


def finish(sel, own_rows, end_rows, own_cols, end_cols, crossed, mine, arrived, per, owners, scale):
    k, vs, shots = own_rows.shape
    rcv = own_cols.shape[3]
    rows = pl.BlockSpec((2, vs, shots), lambda f, sel: (f, 0, 0))
    partial = pl.BlockSpec((1, 2 * vs, per * rcv), lambda f, sel: (f, 0, 0))
    return pl.pallas_call(
        functools.partial(finish_body, scale),
        grid_spec=pltpu.PrefetchScalarGridSpec(
            num_scalar_prefetch=1,
            grid=(k // 2,),
            in_specs=[
                rows,
                rows,
                pl.BlockSpec((per, 2, shots, rcv), lambda f, sel: (sel[1], f, 0, 0)),
                pl.BlockSpec((per, 2, shots, rcv), lambda f, sel: (2 - 2 * sel[0], f, 0, 0)),
                pl.BlockSpec((1, 1, 2 * vs, per * rcv), lambda f, sel: (sel[0], f, 0, 0)),
                partial,
                partial,
            ],
            out_specs=pl.BlockSpec(
                (owners, 1, 2, vs // owners, per * rcv), lambda f, sel: (0, f, 0, 0, 0)
            ),
        ),
        out_shape=jax.ShapeDtypeStruct((owners, k // 2, 2, vs // owners, per * rcv), jnp.bfloat16),
        cost_estimate=pl.CostEstimate(
            flops=8 * k * vs * shots * per * rcv,
            bytes_accessed=2 * k * (2 * vs * shots + 2 * shots * per * rcv + 4 * vs * per * rcv),
            transcendentals=0,
        ),
        name="finish",
    )(sel, own_rows, end_rows, own_cols, end_cols, crossed, mine, arrived)


def gram_by_cycle(rows, sp, per, n_src, n_rcv, scale):
    at = lax.axis_index("src")
    spread = lax.all_gather(rows, "src", axis=0, tiled=False)
    here = [rows]
    cols = [lax.dynamic_slice_in_dim(sp, at * per, per, 0)]
    for d in range(1, n_src):
        here.append(lax.dynamic_index_in_dim(spread, lax.rem(at + n_src - d, n_src), 0, False))
        block = lax.dynamic_slice_in_dim(sp, lax.rem(at + d, n_src) * per, per, 0)
        cols.append(lax.ppermute(block, "src", [(s, (s + d) % n_src) for s in range(n_src)]))
    return gram(here, cols, n_rcv, scale)


def gram_by_halves(rows, sp, per, n_rcv, scale):
    at = lax.axis_index("src")
    low = (at < 2).astype(jnp.int32)
    inner = ((at == 1) | (at == 2)).astype(jnp.int32)
    sel = jnp.stack([low, at.astype(jnp.int32), inner])
    inward = [(0, 1), (3, 2)]
    block = lax.dynamic_slice_in_dim(sp, low * per, 3 * per, 0)
    end_rows = lax.ppermute(rows, "src", inward)
    end_cols = lax.ppermute(block, "src", inward)
    crossed = cross(sel, rows, end_rows, sp, end_cols, per, scale)
    crossed = lax.ppermute(crossed, "src", [(1, 2), (2, 1)])
    mine = onward(sel, rows, sp, crossed, per, scale)
    arrived = lax.ppermute(mine, "src", [(1, 0), (2, 3)])
    return finish(
        sel, rows, end_rows, sp, end_cols, crossed, mine, arrived, per, n_rcv, scale
    )


def chunk_sizes(count):
    return [1] * (count % 2) + ([2] * (count // 2) if count < 8 else [1, 1] + [2] * (count // 2 - 2) + [1, 1])


def shards(traces, index):
    shots, rcv, times = traces.shape
    n_rcv = lax.axis_size("rcv")
    n_src = lax.axis_size("src")
    per = n_rcv // n_src
    vs = index.shape[0]
    scale = 1.0 / math.sqrt(shots * n_src)
    forward, inverse = make_tables(times)
    places = jnp.arange(n_rcv * rcv, dtype=jnp.int32).reshape(n_rcv, 1, rcv)
    hot = (index[None, :, None] == places).astype(jnp.bfloat16)
    spectra = jnp.einsum(
        "kt,srt->ksr", forward.reshape(2 * NF, times), traces, preferred_element_type=jnp.float32
    ).astype(jnp.bfloat16)
    pieces = []
    start = 0
    for fc in chunk_sizes(NF // n_rcv):
        count = n_rcv * 2 * fc
        sp = spectra[start : start + count].reshape(n_rcv, 2 * fc, shots, rcv)
        start += count
        sp = lax.all_to_all(sp, "rcv", split_axis=0, concat_axis=0, tiled=True)
        rows = jnp.einsum("jvr,jksr->kvs", hot, sp, preferred_element_type=jnp.float32)
        rows = rows.astype(jnp.bfloat16)
        if n_src == 4:
            g = gram_by_halves(rows, sp, per, n_rcv, scale)
        else:
            g = gram_by_cycle(rows, sp, per, n_src, n_rcv, scale)
        g = lax.all_to_all(g, "rcv", split_axis=0, concat_axis=0, tiled=True)
        pieces.append(g.reshape(count, vs // n_rcv, per * rcv).transpose(1, 0, 2))
    return lags(pieces, inverse.reshape(2 * NF, times))


def solution(mesh):
    placed = (P("src", "rcv", None), P())

    return jax.shard_map(
        shards, mesh=mesh, in_specs=placed, out_specs=P("rcv", "src", None), check_vma=False
    )
```
